8 devices in a mesh: batch: 1 (over z), cy: 2 (over y), cx: 4 (over x, core).
Axes of the slice: x: 2, y: 2, z: 1, core: 2. Of those that a mesh axis runs over, the one named last changes fastest.
Arguments:
- q_seq: bfloat16 [8192, 16, 256], P(('batch', 'cx', 'cy'))
- k_seq: bfloat16 [8192, 16, 256], P(('batch', 'cx', 'cy'))
- v_seq: bfloat16 [8192, 16, 256], P(('batch', 'cx', 'cy'))
Outputs:
- output: bfloat16 [8192, 16, 256], P(('batch', 'cx', 'cy'))
All inputs are finite; a program needn't handle non-finite values.
Results may differ from the reference program's by a relative error of at most 0.004836.
Values are sent between devices in bfloat16 or wider.
A program may use at most 1 GiB of HBM per device.

```python
import math
import jax
import jax.numpy as jnp
from jax import lax

SEQ = 8192
HEADS = 16
KV_HEADS = 16
HEAD = 256
Q_BLOCK = 32

GROUP_HEADS = HEADS // KV_HEADS
SCORE_STD = math.sqrt(max(1.0, math.log(SEQ / 64.0)))


def setup_inputs(seed: int = 0, part: int = 0) -> dict:
    base_key = jax.random.fold_in(jax.random.key(seed), part)
    key_q, key_k, key_v = jax.random.split(base_key, 3)
    in_scale = math.sqrt(SCORE_STD)
    q_seq = jax.random.normal(key_q, (SEQ, HEADS, HEAD), jnp.float32) * in_scale
    k_seq = jax.random.normal(key_k, (SEQ, KV_HEADS, HEAD), jnp.float32) * in_scale
    v_seq = jax.random.normal(key_v, (SEQ, KV_HEADS, HEAD), jnp.float32) * 2.0
    return {"q_seq": q_seq.astype(jnp.bfloat16), "k_seq": k_seq.astype(jnp.bfloat16), "v_seq": v_seq.astype(jnp.bfloat16)}


def reference(q_seq, k_seq, v_seq):
    score_scale = 1.0 / math.sqrt(HEAD)
    keys_wide = k_seq.astype(jnp.float32)
    vals_wide = v_seq.astype(jnp.float32)
    q_blocks = q_seq.reshape(SEQ // Q_BLOCK, Q_BLOCK, KV_HEADS, GROUP_HEADS, HEAD)

    def attend_block(q_part):
        scores = jnp.einsum("qkgd,skd->kgqs", q_part.astype(jnp.float32), keys_wide) * score_scale
        row_max = jnp.max(scores, axis=-1, keepdims=True)
        prob_all = jnp.exp(scores - row_max)
        row_sum = jnp.sum(prob_all, axis=-1)
        weighted = jnp.einsum("kgqs,skd->qkgd", prob_all.astype(jnp.bfloat16).astype(jnp.float32), vals_wide)
        result = weighted / jnp.transpose(row_sum, (2, 0, 1))[..., None]
        return result.astype(jnp.bfloat16)

    out_blocks = lax.map(attend_block, q_blocks)
    return out_blocks.reshape(SEQ, HEADS, HEAD)
```

```python
import functools
import math
import jax
import jax.numpy as jnp
from jax import lax
from jax.experimental import pallas as pl
from jax.experimental.pallas import tpu as pltpu
from jax.sharding import PartitionSpec as P

MESH = pl.DeviceIdType.MESH
KV_TILE = 512
UNROLL = 2
K_IDX, V_IDX, Q_IDX = 0, 1, 2
SEND_ORDER = (6, 2, 4, 7, 3, 5, 1)


def attend(scale, q, k_at, v_at, num_tiles, row_max, row_sum, out_acc, scores_buf):
    def scores_of(tile):
        return lax.dot_general(q, k_at(tile), (((1,), (1,)), ((), ())), preferred_element_type=jnp.float32)

    row_max[...] = jnp.full_like(row_max, -jnp.inf)
    row_sum[...] = jnp.zeros_like(row_sum)
    out_acc[...] = jnp.zeros_like(out_acc)
    scores_buf[0] = scores_of(0)

    def step(trip, carry):
        for part in range(UNROLL):
            tile = trip * UNROLL + part
            scores_buf[(part + 1) % 2] = scores_of(jnp.minimum(tile + 1, num_tiles - 1))
            scores = scores_buf[part % 2]
            old_max = row_max[...]
            new_max = jnp.maximum(old_max, jnp.max(scores, axis=1, keepdims=True) * scale)
            rescale = jnp.exp2(old_max - new_max)
            prob = jnp.exp2(scores * scale - jnp.tile(new_max, (1, KV_TILE // 128)))
            lanes = prob[:, :128]
            for c in range(1, KV_TILE // 128):
                lanes = lanes + prob[:, c * 128 : (c + 1) * 128]
            row_sum[...] = row_sum[...] * rescale + lanes
            row_max[...] = new_max
            weighted = lax.dot_general(
                prob.astype(jnp.bfloat16), v_at(tile), (((1,), (0,)), ((), ())), preferred_element_type=jnp.float32
            )
            out_acc[...] = out_acc[...] * jnp.tile(rescale, (1, out_acc.shape[1] // 128)) + weighted
        return carry

    lax.fori_loop(0, num_tiles // UNROLL, step, 0)
    total = jnp.sum(row_sum[...], axis=1, keepdims=True)
    return (out_acc[...] / total).astype(jnp.bfloat16)


def kernel(
    k_hbm, v_hbm, q_hbm, o_hbm, k_buf, v_buf, q_buf, o_buf, row_max, row_sum, out_acc, scores_buf, send_sem, recv_sem
):
    heads, tokens, head_dim = k_hbm.shape[1:]
    iy, ix = lax.axis_index("cy"), lax.axis_index("cx")
    me = ix * 2 + iy
    batch = lax.axis_index("batch")
    sources = (k_hbm, v_hbm, q_hbm)
    buffers = (k_buf, v_buf, q_buf)

    def peer(slot):
        px = (ix // 2 + slot // 4) % 2
        pc = (ix % 2 + slot % 2) % 2
        py = (iy + (slot // 2) % 2) % 2
        return px * 2 + pc, py

    def fetch(kind, head, slot):
        cx, cy = peer(slot)
        return pltpu.make_async_remote_copy(
            src_ref=sources[kind].at[cx * 2 + cy, head],
            dst_ref=buffers[kind].at[head, slot],
            send_sem=send_sem.at[kind, head, slot],
            recv_sem=recv_sem.at[kind, head, slot],
            device_id=(batch, cy, cx),
            device_id_type=MESH,
        )

    def fetch_own(kind, head):
        return pltpu.make_async_copy(
            sources[kind].at[me, head], buffers[kind].at[head, 0], recv_sem.at[kind, head, 0]
        )

    def give(head, slot):
        cx, cy = peer(slot)
        return pltpu.make_async_remote_copy(
            src_ref=o_buf.at[head, slot],
            dst_ref=o_hbm.at[me, head],
            send_sem=send_sem.at[3, head, slot],
            recv_sem=recv_sem.at[3, head, slot],
            device_id=(batch, cy, cx),
            device_id_type=MESH,
        )

    def give_own(head):
        return pltpu.make_async_copy(o_buf.at[head, 0], o_hbm.at[me, head], recv_sem.at[3, head, 0])

    barrier = pltpu.get_barrier_semaphore()
    for slot in range(1, 8):
        cx, cy = peer(slot)
        pl.semaphore_signal(barrier, inc=1, device_id=(batch, cy, cx), device_id_type=MESH)
    pl.semaphore_wait(barrier, 7)

    for head in range(heads):
        for kind in (K_IDX, V_IDX, Q_IDX):
            fetch_own(kind, head).start()
            for slot in SEND_ORDER:
                fetch(kind, head, slot).start()

    scale = math.log2(math.e) / math.sqrt(head_dim)
    per_slot = tokens // KV_TILE

    def rows(tile):
        return pl.ds(pl.multiple_of((tile % per_slot) * KV_TILE, KV_TILE), KV_TILE)

    def one_head(head, carry):
        for kind in (K_IDX, V_IDX):
            fetch_own(kind, head).wait()
            for slot in range(1, 8):
                fetch(kind, head, slot).wait_recv()

        def one_slot(turn, carry):
            slot = turn + head * (7 - 2 * turn)

            @pl.when(slot == 0)
            def _():
                fetch_own(Q_IDX, head).wait()

            @pl.when(slot != 0)
            def _():
                fetch(Q_IDX, head, slot).wait_recv()

            o_buf[head, slot] = attend(
                scale,
                q_buf[head, slot],
                lambda tile: k_buf[head, tile // per_slot, rows(tile), :],
                lambda tile: v_buf[head, tile // per_slot, rows(tile), :],
                8 * per_slot,
                row_max,
                row_sum,
                out_acc,
                scores_buf,
            )

            @pl.when(slot == 0)
            def _():
                give_own(head).start()

            @pl.when(slot != 0)
            def _():
                give(head, slot).start()

            return carry

        return lax.fori_loop(0, 8, one_slot, carry)

    lax.fori_loop(0, heads, one_head, 0)

    for head in range(heads):
        give_own(head).wait()
        for slot in range(1, 8):
            for kind in (K_IDX, V_IDX, Q_IDX):
                fetch(kind, head, slot).wait_send()
            give(head, slot).wait_send()
            give(head, slot).wait_recv()


def solution(mesh):
    group = mesh.shape["cx"] * mesh.shape["cy"]
    seq_spec = P(("batch", "cx", "cy"), None, None)

    def local_attention(q_local, k_local, v_local):
        tokens, num_heads, head_dim = q_local.shape
        heads = num_heads // group
        blocks = (heads, group, tokens, head_dim)

        def by_head(x):
            return jnp.transpose(x, (1, 0, 2)).reshape(group, heads, tokens, head_dim)

        out = pl.pallas_call(
            kernel,
            out_shape=jax.ShapeDtypeStruct((group, heads, tokens, head_dim), jnp.bfloat16),
            in_specs=[pl.BlockSpec(memory_space=pl.ANY)] * 3,
            out_specs=pl.BlockSpec(memory_space=pl.ANY),
            scratch_shapes=[
                pltpu.VMEM(blocks, jnp.bfloat16),
                pltpu.VMEM(blocks, jnp.bfloat16),
                pltpu.VMEM(blocks, jnp.bfloat16),
                pltpu.VMEM(blocks, jnp.bfloat16),
                pltpu.VMEM((tokens, 128), jnp.float32),
                pltpu.VMEM((tokens, 128), jnp.float32),
                pltpu.VMEM((tokens, head_dim), jnp.float32),
                pltpu.VMEM((2, tokens, KV_TILE), jnp.float32),
                pltpu.SemaphoreType.DMA((4, heads, group)),
                pltpu.SemaphoreType.DMA((4, heads, group)),
            ],
            compiler_params=pltpu.CompilerParams(
                collective_id=0, has_side_effects=True, vmem_limit_bytes=60 * 2**20
            ),
        )(by_head(k_local), by_head(v_local), by_head(q_local))
        return jnp.transpose(out.reshape(num_heads, tokens, head_dim), (1, 0, 2))

    return jax.shard_map(
        local_attention, mesh=mesh, in_specs=(seq_spec, seq_spec, seq_spec), out_specs=seq_spec, check_vma=False
    )
```

```python
import functools
import math
import jax
import jax.numpy as jnp
from jax import lax
from jax.experimental import pallas as pl
from jax.experimental.pallas import tpu as pltpu
from jax.sharding import PartitionSpec as P

MESH = pl.DeviceIdType.MESH
KV_TILE = 512
UNROLL = 2
TOKEN_TILE = 128
TOKEN_GROUP = 16
K_IDX, V_IDX, Q_IDX = 0, 1, 2
SEND_ORDER = (6, 2, 4, 7, 3, 5, 1)


def attend(scale, q, k_at, v_at, num_tiles, row_max, row_sum, out_acc, scores_buf):
    def scores_of(tile):
        return lax.dot_general(q, k_at(tile), (((1,), (1,)), ((), ())), preferred_element_type=jnp.float32)

    row_max[...] = jnp.full_like(row_max, -jnp.inf)
    row_sum[...] = jnp.zeros_like(row_sum)
    out_acc[...] = jnp.zeros_like(out_acc)
    scores_buf[0] = scores_of(0)

    def step(trip, carry):
        for part in range(UNROLL):
            tile = trip * UNROLL + part
            scores_buf[(part + 1) % 2] = scores_of(jnp.minimum(tile + 1, num_tiles - 1))
            scores = scores_buf[part % 2]
            old_max = row_max[...]
            new_max = jnp.maximum(old_max, jnp.max(scores, axis=1, keepdims=True) * scale)
            rescale = jnp.exp2(old_max - new_max)
            prob = jnp.exp2(scores * scale - jnp.tile(new_max, (1, KV_TILE // 128)))
            lanes = prob[:, :128]
            for c in range(1, KV_TILE // 128):
                lanes = lanes + prob[:, c * 128 : (c + 1) * 128]
            row_sum[...] = row_sum[...] * rescale + lanes
            row_max[...] = new_max
            weighted = lax.dot_general(
                prob.astype(jnp.bfloat16), v_at(tile), (((1,), (0,)), ((), ())), preferred_element_type=jnp.float32
            )
            out_acc[...] = out_acc[...] * jnp.tile(rescale, (1, out_acc.shape[1] // 128)) + weighted
        return carry

    lax.fori_loop(0, num_tiles // UNROLL, step, 0)
    total = jnp.sum(row_sum[...], axis=1, keepdims=True)
    return (out_acc[...] / total).astype(jnp.bfloat16)


def kernel(
    k_hbm, v_hbm, q_hbm, o_hbm,
    k_buf, v_buf, q_buf, stage, landing, row_max, row_sum, out_acc, scores_buf, send_sem, recv_sem, load_sem,
):
    heads, group, tokens, head_dim = k_buf.shape
    iy, ix = lax.axis_index("cy"), lax.axis_index("cx")
    me = ix * 2 + iy
    batch = lax.axis_index("batch")
    sources = (k_hbm, v_hbm, q_hbm)
    buffers = (k_buf, v_buf, q_buf)
    num_loads = tokens // TOKEN_TILE

    def peer(slot):
        px = (ix // 2 + slot // 4) % 2
        pc = (ix % 2 + slot % 2) % 2
        py = (iy + (slot // 2) % 2) % 2
        return px * 2 + pc, py

    def fetch(kind, head, slot, span=slice(None)):
        cx, cy = peer(slot)
        return pltpu.make_async_remote_copy(
            src_ref=stage.at[kind, cx * 2 + cy, head, span],
            dst_ref=buffers[kind].at[head, slot, span],
            send_sem=send_sem.at[kind, head, slot],
            recv_sem=recv_sem.at[kind, head, slot],
            device_id=(batch, cy, cx),
            device_id_type=MESH,
        )

    def fetch_own(kind, head):
        return pltpu.make_async_copy(
            stage.at[kind, me, head], buffers[kind].at[head, 0], recv_sem.at[kind, head, 0]
        )

    def fetch_all(kind, head):
        fetch_own(kind, head).start()
        for slot in SEND_ORDER:
            fetch(kind, head, slot).start()

    def give(head, slot):
        cx, cy = peer(slot)
        return pltpu.make_async_remote_copy(
            src_ref=stage.at[K_IDX, cx * 2 + cy, head],
            dst_ref=o_hbm.at[me, head],
            send_sem=send_sem.at[3, head, slot],
            recv_sem=recv_sem.at[3, head, slot],
            device_id=(batch, cy, cx),
            device_id_type=MESH,
        )

    def give_own(head):
        return pltpu.make_async_copy(stage.at[K_IDX, me, head], o_hbm.at[me, head], recv_sem.at[3, head, 0])

    def token_span(tile):
        return pl.ds(pl.multiple_of(tile * TOKEN_TILE, TOKEN_TILE), TOKEN_TILE)

    def load(kind, tile):
        return pltpu.make_async_copy(
            sources[kind].at[token_span(tile)], landing.at[tile % 2], load_sem.at[tile % 2]
        )

    load(K_IDX, 0).start()
    barrier = pltpu.get_barrier_semaphore()
    for slot in range(1, 8):
        cx, cy = peer(slot)
        pl.semaphore_signal(barrier, inc=1, device_id=(batch, cy, cx), device_id_type=MESH)
    pl.semaphore_wait(barrier, 7)

    def send_first(tile):
        for slot in SEND_ORDER:
            fetch(K_IDX, 0, slot, token_span(tile)).start()

    for kind in (K_IDX, V_IDX, Q_IDX):

        def relayout(tile, carry):
            @pl.when(tile + 1 < num_loads)
            def _():
                load(kind, tile + 1).start()

            if kind != Q_IDX:

                @pl.when(tile + 1 == num_loads)
                def _():
                    load(kind + 1, 0).start()

            load(kind, tile).wait()

            def some_tokens(part, carry):
                rows = pl.ds(pl.multiple_of(part * TOKEN_GROUP, TOKEN_GROUP), TOKEN_GROUP)
                first = pl.multiple_of(tile * TOKEN_TILE + part * TOKEN_GROUP, TOKEN_GROUP)
                by_head = jnp.swapaxes(landing[tile % 2, rows], 0, 1)
                stage[kind, :, :, pl.ds(first, TOKEN_GROUP), :] = by_head.reshape(group, heads, TOKEN_GROUP, head_dim)
                return carry

            lax.fori_loop(0, TOKEN_TILE // TOKEN_GROUP, some_tokens, 0)

            if kind == K_IDX:

                @pl.when(tile > 0)
                def _():
                    send_first(tile - 1)

            return carry

        lax.fori_loop(0, num_loads, relayout, 0)
        if kind == V_IDX:
            send_first(num_loads - 1)
            fetch_own(K_IDX, 0).start()

    for kind, head in ((V_IDX, 0), (Q_IDX, 0), (K_IDX, 1), (V_IDX, 1), (Q_IDX, 1)):
        fetch_all(kind, head)

    scale = math.log2(math.e) / math.sqrt(head_dim)
    per_slot = tokens // KV_TILE

    def rows(tile):
        return pl.ds(pl.multiple_of((tile % per_slot) * KV_TILE, KV_TILE), KV_TILE)

    def one_head(head, carry):
        for kind in (K_IDX, V_IDX):
            fetch_own(kind, head).wait()
            for slot in range(1, 8):
                fetch(kind, head, slot).wait_recv()

        def one_slot(turn, carry):
            slot = turn + head * (7 - 2 * turn)
            cx, cy = peer(slot)

            @pl.when(slot == 0)
            def _():
                fetch_own(Q_IDX, head).wait()

            @pl.when(slot != 0)
            def _():
                fetch(Q_IDX, head, slot).wait_recv()
                fetch(K_IDX, head, slot).wait_send()

            stage[K_IDX, cx * 2 + cy, head] = attend(
                scale,
                q_buf[head, slot],
                lambda tile: k_buf[head, tile // per_slot, rows(tile), :],
                lambda tile: v_buf[head, tile // per_slot, rows(tile), :],
                8 * per_slot,
                row_max,
                row_sum,
                out_acc,
                scores_buf,
            )

            @pl.when(slot == 0)
            def _():
                give_own(head).start()

            @pl.when(slot != 0)
            def _():
                give(head, slot).start()

            return carry

        return lax.fori_loop(0, 8, one_slot, carry)

    lax.fori_loop(0, heads, one_head, 0)

    for head in range(heads):
        give_own(head).wait()
        for slot in range(1, 8):
            for kind in (V_IDX, Q_IDX):
                fetch(kind, head, slot).wait_send()
            give(head, slot).wait_send()
            give(head, slot).wait_recv()


def by_token(o_hbm, out_hbm, o_buf, out_buf, in_sem, out_sem):
    num_tiles = o_hbm.shape[1] // TOKEN_TILE

    def span(tile):
        return pl.ds(pl.multiple_of(tile * TOKEN_TILE, TOKEN_TILE), TOKEN_TILE)

    def take(tile):
        return pltpu.make_async_copy(o_hbm.at[:, span(tile)], o_buf.at[:, span(tile)], in_sem.at[tile])

    def put(tile):
        return pltpu.make_async_copy(out_buf.at[span(tile)], out_hbm.at[span(tile)], out_sem.at[tile])

    for tile in range(num_tiles):
        take(tile).start()

    def one_tile(tile, carry):
        take(tile).wait()

        def some_tokens(part, carry):
            rows = pl.ds(pl.multiple_of(tile * TOKEN_TILE + part * TOKEN_GROUP, TOKEN_GROUP), TOKEN_GROUP)
            out_buf[rows] = jnp.swapaxes(o_buf[:, rows], 0, 1)
            return carry

        lax.fori_loop(0, TOKEN_TILE // TOKEN_GROUP, some_tokens, 0)
        put(tile).start()
        return carry

    lax.fori_loop(0, num_tiles, one_tile, 0)
    for tile in range(num_tiles):
        put(tile).wait()


def solution(mesh):
    group = mesh.shape["cx"] * mesh.shape["cy"]
    seq_spec = P(("batch", "cx", "cy"), None, None)

    def local_attention(q_local, k_local, v_local):
        tokens, num_heads, head_dim = q_local.shape
        heads = num_heads // group
        blocks = (heads, group, tokens, head_dim)
        anywhere = pl.BlockSpec(memory_space=pl.ANY)

        out = pl.pallas_call(
            kernel,
            out_shape=jax.ShapeDtypeStruct((group, heads, tokens, head_dim), jnp.bfloat16),
            in_specs=[anywhere] * 3,
            out_specs=anywhere,
            scratch_shapes=[
                pltpu.VMEM(blocks, jnp.bfloat16),
                pltpu.VMEM(blocks, jnp.bfloat16),
                pltpu.VMEM(blocks, jnp.bfloat16),
                pltpu.VMEM((3, group, heads, tokens, head_dim), jnp.bfloat16),
                pltpu.VMEM((2, TOKEN_TILE, num_heads, head_dim), jnp.bfloat16),
                pltpu.VMEM((tokens, 128), jnp.float32),
                pltpu.VMEM((tokens, 128), jnp.float32),
                pltpu.VMEM((tokens, head_dim), jnp.float32),
                pltpu.VMEM((2, tokens, KV_TILE), jnp.float32),
                pltpu.SemaphoreType.DMA((4, heads, group)),
                pltpu.SemaphoreType.DMA((4, heads, group)),
                pltpu.SemaphoreType.DMA((2,)),
            ],
            compiler_params=pltpu.CompilerParams(
                collective_id=0, has_side_effects=True, vmem_limit_bytes=67043328
            ),
        )(k_local, v_local, q_local)
        return pl.pallas_call(
            by_token,
            out_shape=jax.ShapeDtypeStruct(q_local.shape, jnp.bfloat16),
            in_specs=[anywhere],
            out_specs=anywhere,
            scratch_shapes=[
                pltpu.VMEM((num_heads, tokens, head_dim), jnp.bfloat16),
                pltpu.VMEM((tokens, num_heads, head_dim), jnp.bfloat16),
                pltpu.SemaphoreType.DMA((tokens // TOKEN_TILE,)),
                pltpu.SemaphoreType.DMA((tokens // TOKEN_TILE,)),
            ],
            compiler_params=pltpu.CompilerParams(vmem_limit_bytes=48 * 2**20),
        )(out.reshape(num_heads, tokens, head_dim))

    return jax.shard_map(
        local_attention, mesh=mesh, in_specs=(seq_spec, seq_spec, seq_spec), out_specs=seq_spec, check_vma=False
    )
```

```python
import functools
import math
import jax
import jax.numpy as jnp
from jax import lax
from jax.experimental import pallas as pl
from jax.experimental.pallas import tpu as pltpu
from jax.sharding import PartitionSpec as P

MESH = pl.DeviceIdType.MESH
KV_TILE = 512
UNROLL = 4
TOKEN_TILE = 128
LOAD_TILE = 64
TOKEN_GROUP = 16
K_IDX, V_IDX, Q_IDX = 0, 1, 2
SEND_ORDER = (6, 2, 4, 7, 3, 5, 1)


def attend(scale, q_at, k_at, v_at, num_tiles, row_max, row_sum, out_acc, scores_buf):
    def scores_of(tile):
        return lax.dot_general(q_at(), k_at(tile), (((1,), (1,)), ((), ())), preferred_element_type=jnp.float32)

    row_max[...] = jnp.full_like(row_max, -jnp.inf)
    row_sum[...] = jnp.zeros_like(row_sum)
    out_acc[...] = jnp.zeros_like(out_acc)
    scores_buf[0] = scores_of(0)

    def step(trip, carry):
        for part in range(UNROLL):
            tile = trip * UNROLL + part
            scores_buf[(part + 1) % 2] = scores_of(jnp.minimum(tile + 1, num_tiles - 1))
            scores = scores_buf[part % 2]
            old_max = row_max[...]
            new_max = jnp.maximum(old_max, jnp.max(scores, axis=1, keepdims=True) * scale)
            rescale = jnp.exp2(old_max - new_max)
            prob = jnp.exp2(scores * scale - jnp.tile(new_max, (1, KV_TILE // 128)))
            lanes = prob[:, :128]
            for c in range(1, KV_TILE // 128):
                lanes = lanes + prob[:, c * 128 : (c + 1) * 128]
            row_sum[...] = row_sum[...] * rescale + lanes
            row_max[...] = new_max
            weighted = lax.dot_general(
                prob.astype(jnp.bfloat16), v_at(tile), (((1,), (0,)), ((), ())), preferred_element_type=jnp.float32
            )
            out_acc[...] = out_acc[...] * jnp.tile(rescale, (1, out_acc.shape[1] // 128)) + weighted
        return carry

    lax.fori_loop(0, num_tiles // UNROLL, step, 0)
    total = jnp.sum(row_sum[...], axis=1, keepdims=True)
    return (out_acc[...] / total).astype(jnp.bfloat16)


def kernel(
    k_hbm, v_hbm, q_hbm, o_home, pool, landing, row_max, row_sum, out_acc, scores_buf, send_sem, recv_sem, load_sem
):
    group, heads, tokens, head_dim = o_home.shape
    iy, ix = lax.axis_index("cy"), lax.axis_index("cx")
    me = ix * 2 + iy
    batch = lax.axis_index("batch")
    sources = (k_hbm, v_hbm, q_hbm)
    num_loads = tokens // LOAD_TILE

    def peer(slot):
        px = (ix // 2 + slot // 4) % 2
        pc = (ix % 2 + slot % 2) % 2
        py = (iy + (slot // 2) % 2) % 2
        return px * 2 + pc, py

    def block_of(slot):
        return (slot + group - 1) % (2 * group - 1) + (group - slot) // group * (me - group + 1)

    def fetch(kind, head, slot, span=slice(None)):
        cx, cy = peer(slot)
        return pltpu.make_async_remote_copy(
            src_ref=pool.at[kind, cx * 2 + cy, head, span],
            dst_ref=pool.at[kind, group - 1 + slot, head, span],
            send_sem=send_sem.at[kind, head, slot],
            recv_sem=recv_sem.at[kind, head, slot],
            device_id=(batch, cy, cx),
            device_id_type=MESH,
        )

    def fetch_all(kind, head):
        for slot in SEND_ORDER:
            fetch(kind, head, slot).start()

    def give(head, slot):
        cx, cy = peer(slot)
        return pltpu.make_async_remote_copy(
            src_ref=pool.at[Q_IDX, block_of(slot), head],
            dst_ref=o_home.at[me, head],
            send_sem=send_sem.at[3, head, slot],
            recv_sem=recv_sem.at[3, head, slot],
            device_id=(batch, cy, cx),
            device_id_type=MESH,
        )

    def give_own(head):
        return pltpu.make_async_copy(pool.at[Q_IDX, me, head], o_home.at[me, head], recv_sem.at[3, head, 0])

    def token_span(tile):
        return pl.ds(pl.multiple_of(tile * LOAD_TILE, LOAD_TILE), LOAD_TILE)

    def load(kind, tile):
        return pltpu.make_async_copy(
            sources[kind].at[token_span(tile)], landing.at[tile % 2], load_sem.at[tile % 2]
        )

    load(K_IDX, 0).start()
    barrier = pltpu.get_barrier_semaphore()
    for slot in range(1, 8):
        cx, cy = peer(slot)
        pl.semaphore_signal(barrier, inc=1, device_id=(batch, cy, cx), device_id_type=MESH)

    def send_first(tile):
        for slot in SEND_ORDER:
            fetch(K_IDX, 0, slot, token_span(tile)).start()

    for kind in (K_IDX, V_IDX, Q_IDX):

        def relayout(tile, carry):
            @pl.when(tile + 1 < num_loads)
            def _():
                load(kind, tile + 1).start()

            if kind != Q_IDX:

                @pl.when(tile + 1 == num_loads)
                def _():
                    load(kind + 1, 0).start()

            load(kind, tile).wait()

            def some_tokens(part, carry):
                rows = pl.ds(pl.multiple_of(part * TOKEN_GROUP, TOKEN_GROUP), TOKEN_GROUP)
                first = pl.multiple_of(tile * LOAD_TILE + part * TOKEN_GROUP, TOKEN_GROUP)
                by_head = jnp.swapaxes(landing[tile % 2, rows], 0, 1)
                pool[kind, :group, :, pl.ds(first, TOKEN_GROUP), :] = by_head.reshape(
                    group, heads, TOKEN_GROUP, head_dim
                )
                return carry

            lax.fori_loop(0, LOAD_TILE // TOKEN_GROUP, some_tokens, 0)

            if kind == K_IDX:

                @pl.when(tile == 0)
                def _():
                    pl.semaphore_wait(barrier, 7)

                @pl.when(tile > 0)
                def _():
                    send_first(tile - 1)

            return carry

        lax.fori_loop(0, num_loads, relayout, 0)
        if kind == V_IDX:
            send_first(num_loads - 1)

    for kind, head in ((V_IDX, 0), (Q_IDX, 0), (K_IDX, 1), (V_IDX, 1), (Q_IDX, 1)):
        fetch_all(kind, head)

    scale = math.log2(math.e) / math.sqrt(head_dim)
    per_slot = tokens // KV_TILE

    def rows(tile):
        return pl.ds(pl.multiple_of((tile % per_slot) * KV_TILE, KV_TILE), KV_TILE)

    def one_head(head, carry):
        for kind in (K_IDX, V_IDX):
            for slot in range(1, 8):
                fetch(kind, head, slot).wait_recv()

        @pl.when(head > 0)
        def _():
            give_own(head - 1).start()
            for slot in SEND_ORDER:
                give(head - 1, slot).start()

        def one_slot(turn, carry):
            slot = turn + head * (7 - 2 * turn)
            block = block_of(slot)

            @pl.when(slot != 0)
            def _():
                fetch(Q_IDX, head, slot).wait_recv()

            pool[Q_IDX, block, head] = attend(
                scale,
                lambda: pool[Q_IDX, block, head],
                lambda tile: pool[K_IDX, block_of(tile // per_slot), head, rows(tile), :],
                lambda tile: pool[V_IDX, block_of(tile // per_slot), head, rows(tile), :],
                group * per_slot,
                row_max,
                row_sum,
                out_acc,
                scores_buf,
            )

            @pl.when((head == heads - 1) & (slot == 0))
            def _():
                give_own(head).start()

            @pl.when((head == heads - 1) & (slot != 0))
            def _():
                give(head, slot).start()

            return carry

        return lax.fori_loop(0, 8, one_slot, carry)

    lax.fori_loop(0, heads, one_head, 0)

    for head in range(heads):
        give_own(head).wait()
        for slot in range(1, 8):
            for kind in (K_IDX, V_IDX, Q_IDX):
                fetch(kind, head, slot).wait_send()
            give(head, slot).wait_send()
            give(head, slot).wait_recv()


def by_token(o_buf, out_hbm, out_buf, out_sem):
    num_tiles = o_buf.shape[1] // TOKEN_TILE

    def put(tile):
        span = pl.ds(pl.multiple_of(tile * TOKEN_TILE, TOKEN_TILE), TOKEN_TILE)
        return pltpu.make_async_copy(out_buf.at[span], out_hbm.at[span], out_sem.at[tile])

    def one_tile(tile, carry):
        def some_tokens(part, carry):
            rows = pl.ds(pl.multiple_of(tile * TOKEN_TILE + part * TOKEN_GROUP, TOKEN_GROUP), TOKEN_GROUP)
            out_buf[rows] = jnp.swapaxes(o_buf[:, rows], 0, 1)
            return carry

        lax.fori_loop(0, TOKEN_TILE // TOKEN_GROUP, some_tokens, 0)
        put(tile).start()
        return carry

    lax.fori_loop(0, num_tiles, one_tile, 0)
    for tile in range(num_tiles):
        put(tile).wait()


def solution(mesh):
    group = mesh.shape["cx"] * mesh.shape["cy"]
    seq_spec = P(("batch", "cx", "cy"), None, None)

    def local_attention(q_local, k_local, v_local):
        tokens, num_heads, head_dim = q_local.shape
        heads = num_heads // group
        blocks = (group, heads, tokens, head_dim)
        anywhere = pl.BlockSpec(memory_space=pl.ANY)

        out = pl.pallas_call(
            kernel,
            out_shape=pltpu.VMEM(blocks, jnp.bfloat16),
            in_specs=[anywhere] * 3,
            out_specs=anywhere,
            scratch_shapes=[
                pltpu.VMEM((3, 2 * group - 1, heads, tokens, head_dim), jnp.bfloat16),
                pltpu.VMEM((2, LOAD_TILE, num_heads, head_dim), jnp.bfloat16),
                pltpu.VMEM((tokens, 128), jnp.float32),
                pltpu.VMEM((tokens, 128), jnp.float32),
                pltpu.VMEM((tokens, head_dim), jnp.float32),
                pltpu.VMEM((2, tokens, KV_TILE), jnp.float32),
                pltpu.SemaphoreType.DMA((4, heads, group)),
                pltpu.SemaphoreType.DMA((4, heads, group)),
                pltpu.SemaphoreType.DMA((2,)),
            ],
            compiler_params=pltpu.CompilerParams(
                collective_id=0, has_side_effects=True, vmem_limit_bytes=58600000
            ),
        )(k_local, v_local, q_local)
        return pl.pallas_call(
            by_token,
            out_shape=jax.ShapeDtypeStruct(q_local.shape, jnp.bfloat16),
            in_specs=[pl.BlockSpec(memory_space=pltpu.VMEM)],
            out_specs=anywhere,
            scratch_shapes=[
                pltpu.VMEM((tokens, num_heads, head_dim), jnp.bfloat16),
                pltpu.SemaphoreType.DMA((tokens // TOKEN_TILE,)),
            ],
            compiler_params=pltpu.CompilerParams(vmem_limit_bytes=24 * 2**20),
        )(out.reshape(num_heads, tokens, head_dim))

    return jax.shard_map(
        local_attention, mesh=mesh, in_specs=(seq_spec, seq_spec, seq_spec), out_specs=seq_spec, check_vma=False
    )
```

```python
import functools
import math
import jax
import jax.numpy as jnp
from jax import lax
from jax.experimental import pallas as pl
from jax.experimental.pallas import tpu as pltpu
from jax.sharding import PartitionSpec as P

MESH = pl.DeviceIdType.MESH
KV_TILE = 512
UNROLL = 4
TOKEN_TILE = 64
LOAD_TILE = 64
TOKEN_GROUP = 16
K_IDX, V_IDX, Q_IDX = 0, 1, 2
SEND_ORDER = (6, 2, 4, 7, 3, 5, 1)


def attend(scale, q_at, k_at, v_at, num_tiles, row_max, row_sum, out_acc, scores_buf):
    def scores_of(tile):
        return lax.dot_general(q_at(), k_at(tile), (((1,), (1,)), ((), ())), preferred_element_type=jnp.float32)

    row_max[...] = jnp.full_like(row_max, jnp.finfo(jnp.float32).min)
    row_sum[...] = jnp.zeros_like(row_sum)
    out_acc[...] = jnp.zeros_like(out_acc)
    scores_buf[0] = scores_of(0)

    def step(trip, carry):
        for part in range(UNROLL):
            tile = trip * UNROLL + part
            scores_buf[(part + 1) % 2] = scores_of(jnp.minimum(tile + 1, num_tiles - 1))
            scores = scores_buf[part % 2]
            old_max = row_max[...]
            new_max = jnp.maximum(old_max, jnp.max(scores, axis=1, keepdims=True))
            rescale = jnp.exp2((old_max - new_max) * scale)
            prob = jnp.exp2((scores - jnp.tile(new_max, (1, KV_TILE // 128))) * scale)
            lanes = prob[:, :128]
            for c in range(1, KV_TILE // 128):
                lanes = lanes + prob[:, c * 128 : (c + 1) * 128]
            row_sum[...] = row_sum[...] * rescale + lanes
            row_max[...] = new_max
            weighted = lax.dot_general(
                prob.astype(jnp.bfloat16), v_at(tile), (((1,), (0,)), ((), ())), preferred_element_type=jnp.float32
            )
            out_acc[...] = out_acc[...] * jnp.tile(rescale, (1, out_acc.shape[1] // 128)) + weighted
        return carry

    lax.fori_loop(0, num_tiles // UNROLL, step, 0)
    total = jnp.sum(row_sum[...], axis=1, keepdims=True)
    return (out_acc[...] / total).astype(jnp.bfloat16)


def kernel(
    k_hbm, v_hbm, q_hbm, o_home, pool, landing, row_max, row_sum, out_acc, scores_buf, send_sem, recv_sem, load_sem
):
    group, heads, tokens, head_dim = o_home.shape
    iy, ix = lax.axis_index("cy"), lax.axis_index("cx")
    me = ix * 2 + iy
    batch = lax.axis_index("batch")
    sources = (k_hbm, v_hbm, q_hbm)
    num_loads = tokens // LOAD_TILE

    def peer(slot):
        px = (ix // 2 + slot // 4) % 2
        pc = (ix % 2 + slot % 2) % 2
        py = (iy + (slot // 2) % 2) % 2
        return px * 2 + pc, py

    def block_of(slot):
        return (slot + group - 1) % (2 * group - 1) + (group - slot) // group * (me - group + 1)

    def fetch(kind, head, slot, span=slice(None)):
        cx, cy = peer(slot)
        return pltpu.make_async_remote_copy(
            src_ref=pool.at[kind, cx * 2 + cy, head, span],
            dst_ref=pool.at[kind, group - 1 + slot, head, span],
            send_sem=send_sem.at[kind, head, slot],
            recv_sem=recv_sem.at[kind, head, slot],
            device_id=(batch, cy, cx),
            device_id_type=MESH,
        )

    def fetch_all(kind, head):
        for slot in SEND_ORDER:
            fetch(kind, head, slot).start()

    def give(head, slot):
        cx, cy = peer(slot)
        return pltpu.make_async_remote_copy(
            src_ref=pool.at[Q_IDX, block_of(slot), head],
            dst_ref=o_home.at[me, head],
            send_sem=send_sem.at[3, head, slot],
            recv_sem=recv_sem.at[3, head, slot],
            device_id=(batch, cy, cx),
            device_id_type=MESH,
        )

    def give_own(head):
        return pltpu.make_async_copy(pool.at[Q_IDX, me, head], o_home.at[me, head], recv_sem.at[3, head, 0])

    def token_span(tile):
        return pl.ds(pl.multiple_of(tile * LOAD_TILE, LOAD_TILE), LOAD_TILE)

    def load(kind, tile):
        return pltpu.make_async_copy(
            sources[kind].at[token_span(tile)], landing.at[tile % 2], load_sem.at[tile % 2]
        )

    load(K_IDX, 0).start()
    barrier = pltpu.get_barrier_semaphore()
    for slot in range(1, 8):
        cx, cy = peer(slot)
        pl.semaphore_signal(barrier, inc=1, device_id=(batch, cy, cx), device_id_type=MESH)

    def send_first(tile, count):
        for slot in SEND_ORDER:
            fetch(K_IDX, 0, slot, pl.ds(tile * LOAD_TILE, count * LOAD_TILE)).start()

    first_spans = [(0, 1)] + [(1 << n, 1 << n) for n in range(num_loads.bit_length() - 1)]

    for kind in (K_IDX, V_IDX, Q_IDX):

        def relayout(tile, carry):
            @pl.when(tile + 1 < num_loads)
            def _():
                load(kind, tile + 1).start()

            if kind != Q_IDX:

                @pl.when(tile + 1 == num_loads)
                def _():
                    load(kind + 1, 0).start()

            load(kind, tile).wait()

            def some_tokens(part, carry):
                rows = pl.ds(pl.multiple_of(part * TOKEN_GROUP, TOKEN_GROUP), TOKEN_GROUP)
                first = pl.multiple_of(tile * LOAD_TILE + part * TOKEN_GROUP, TOKEN_GROUP)
                by_head = jnp.swapaxes(landing[tile % 2, rows], 0, 1)
                pool[kind, :group, :, pl.ds(first, TOKEN_GROUP), :] = by_head.reshape(
                    group, heads, TOKEN_GROUP, head_dim
                )
                return carry

            lax.fori_loop(0, LOAD_TILE // TOKEN_GROUP, some_tokens, 0)

            if kind == K_IDX:

                @pl.when(tile == 1)
                def _():
                    pl.semaphore_wait(barrier, 7)

                for begin, count in first_spans[:-1]:

                    @pl.when(tile == begin + count)
                    def _():
                        send_first(begin, count)

            if kind == V_IDX:

                @pl.when(tile == 0)
                def _():
                    send_first(*first_spans[-1])

            return carry

        lax.fori_loop(0, num_loads, relayout, 0)

    for kind, head in ((V_IDX, 0), (Q_IDX, 0), (K_IDX, 1), (V_IDX, 1), (Q_IDX, 1)):
        fetch_all(kind, head)

    scale = math.log2(math.e) / math.sqrt(head_dim)
    per_slot = tokens // KV_TILE

    def rows(tile):
        return pl.ds(pl.multiple_of((tile % per_slot) * KV_TILE, KV_TILE), KV_TILE)

    def one_head(head, carry):
        for kind in (K_IDX, V_IDX):
            for slot in range(1, 8):
                fetch(kind, head, slot).wait_recv()

        @pl.when(head > 0)
        def _():
            give_own(head - 1).start()
            for slot in SEND_ORDER:
                give(head - 1, slot).start()

        def one_slot(turn, carry):
            slot = turn + head * (7 - 2 * turn)
            block = block_of(slot)

            @pl.when(slot != 0)
            def _():
                fetch(Q_IDX, head, slot).wait_recv()

            pool[Q_IDX, block, head] = attend(
                scale,
                lambda: pool[Q_IDX, block, head],
                lambda tile: pool[K_IDX, block_of(tile // per_slot), head, rows(tile), :],
                lambda tile: pool[V_IDX, block_of(tile // per_slot), head, rows(tile), :],
                group * per_slot,
                row_max,
                row_sum,
                out_acc,
                scores_buf,
            )

            @pl.when((head == heads - 1) & (slot == 0))
            def _():
                give_own(head).start()

            @pl.when((head == heads - 1) & (turn > 0))
            def _():
                give(head, slot + 1).start()

            return carry

        return lax.fori_loop(0, 8, one_slot, carry)

    lax.fori_loop(0, heads, one_head, 0)

    for head in range(heads):
        give_own(head).wait()
        for slot in range(1, 8):
            for kind in (K_IDX, V_IDX, Q_IDX):
                fetch(kind, head, slot).wait_send()
            give(head, slot).wait_send()
            give(head, slot).wait_recv()


def by_token(o_buf, out_hbm, out_buf, out_sem):
    num_tiles = o_buf.shape[1] // TOKEN_TILE

    def put(tile):
        span = pl.ds(pl.multiple_of(tile * TOKEN_TILE, TOKEN_TILE), TOKEN_TILE)
        return pltpu.make_async_copy(out_buf.at[span], out_hbm.at[span], out_sem.at[tile])

    def one_tile(tile, carry):
        def some_tokens(part, carry):
            rows = pl.ds(pl.multiple_of(tile * TOKEN_TILE + part * TOKEN_GROUP, TOKEN_GROUP), TOKEN_GROUP)
            out_buf[rows] = jnp.swapaxes(o_buf[:, rows], 0, 1)
            return carry

        lax.fori_loop(0, TOKEN_TILE // TOKEN_GROUP, some_tokens, 0, unroll=2)
        put(tile).start()
        return carry

    lax.fori_loop(0, num_tiles, one_tile, 0)
    for tile in range(num_tiles):
        put(tile).wait()


def solution(mesh):
    group = mesh.shape["cx"] * mesh.shape["cy"]
    seq_spec = P(("batch", "cx", "cy"), None, None)

    def local_attention(q_local, k_local, v_local):
        tokens, num_heads, head_dim = q_local.shape
        heads = num_heads // group
        blocks = (group, heads, tokens, head_dim)
        anywhere = pl.BlockSpec(memory_space=pl.ANY)

        out = pl.pallas_call(
            kernel,
            out_shape=pltpu.VMEM(blocks, jnp.bfloat16),
            in_specs=[anywhere] * 3,
            out_specs=anywhere,
            scratch_shapes=[
                pltpu.VMEM((3, 2 * group - 1, heads, tokens, head_dim), jnp.bfloat16),
                pltpu.VMEM((2, LOAD_TILE, num_heads, head_dim), jnp.bfloat16),
                pltpu.VMEM((tokens, 128), jnp.float32),
                pltpu.VMEM((tokens, 128), jnp.float32),
                pltpu.VMEM((tokens, head_dim), jnp.float32),
                pltpu.VMEM((2, tokens, KV_TILE), jnp.float32),
                pltpu.SemaphoreType.DMA((4, heads, group)),
                pltpu.SemaphoreType.DMA((4, heads, group)),
                pltpu.SemaphoreType.DMA((2,)),
            ],
            compiler_params=pltpu.CompilerParams(
                collective_id=0, has_side_effects=True, vmem_limit_bytes=58600000
            ),
        )(k_local, v_local, q_local)
        return pl.pallas_call(
            by_token,
            out_shape=jax.ShapeDtypeStruct(q_local.shape, jnp.bfloat16),
            in_specs=[pl.BlockSpec(memory_space=pltpu.VMEM)],
            out_specs=anywhere,
            scratch_shapes=[
                pltpu.VMEM((tokens, num_heads, head_dim), jnp.bfloat16),
                pltpu.SemaphoreType.DMA((tokens // TOKEN_TILE,)),
            ],
            compiler_params=pltpu.CompilerParams(vmem_limit_bytes=24 * 2**20),
        )(out.reshape(num_heads, tokens, head_dim))

    return jax.shard_map(
        local_attention, mesh=mesh, in_specs=(seq_spec, seq_spec, seq_spec), out_specs=seq_spec, check_vma=False
    )
```

```python
import functools
import math
import jax
import jax.numpy as jnp
from jax import lax
from jax.experimental import pallas as pl
from jax.experimental.pallas import tpu as pltpu
from jax.sharding import PartitionSpec as P

MESH = pl.DeviceIdType.MESH
KV_TILE = 512
UNROLL = 4
TOKEN_TILE = 64
LOAD_TILE = 64
TOKEN_GROUP = 16
K_IDX, V_IDX, Q_IDX = 0, 1, 2
SEND_ORDER = (6, 2, 4, 7, 3, 5, 1)


def attend(scale, q_at, k_at, v_at, num_tiles, row_max, row_sum, out_acc, scores_buf):
    def scores_of(tile):
        return lax.dot_general(q_at(), k_at(tile), (((1,), (1,)), ((), ())), preferred_element_type=jnp.float32)

    row_max[...] = jnp.full_like(row_max, jnp.finfo(jnp.float32).min)
    row_sum[...] = jnp.zeros_like(row_sum)
    out_acc[...] = jnp.zeros_like(out_acc)
    scores_buf[0] = scores_of(0)

    def step(trip, carry):
        for part in range(UNROLL):
            tile = trip * UNROLL + part
            scores_buf[(part + 1) % 2] = scores_of(jnp.minimum(tile + 1, num_tiles - 1))
            scores = scores_buf[part % 2]
            old_max = row_max[...]
            new_max = jnp.maximum(old_max, jnp.max(scores, axis=1, keepdims=True))
            rescale = jnp.exp2((old_max - new_max) * scale)
            prob = jnp.exp2((scores - jnp.tile(new_max, (1, KV_TILE // 128))) * scale)
            lanes = prob[:, :128]
            for c in range(1, KV_TILE // 128):
                lanes = lanes + prob[:, c * 128 : (c + 1) * 128]
            row_sum[...] = row_sum[...] * rescale + lanes
            row_max[...] = new_max
            weighted = lax.dot_general(
                prob.astype(jnp.bfloat16), v_at(tile), (((1,), (0,)), ((), ())), preferred_element_type=jnp.float32
            )
            out_acc[...] = out_acc[...] * jnp.tile(rescale, (1, out_acc.shape[1] // 128)) + weighted
        return carry

    lax.fori_loop(0, num_tiles // UNROLL, step, 0)
    total = jnp.sum(row_sum[...], axis=1, keepdims=True)
    return (out_acc[...] / total).astype(jnp.bfloat16)


def kernel(
    k_hbm, v_hbm, q_hbm, o_home, pool, landing, row_max, row_sum, out_acc, scores_buf, send_sem, recv_sem, load_sem
):
    group, heads, tokens, head_dim = o_home.shape
    iy, ix = lax.axis_index("cy"), lax.axis_index("cx")
    me = ix * 2 + iy
    batch = lax.axis_index("batch")
    sources = (k_hbm, v_hbm, q_hbm)
    num_loads = tokens // LOAD_TILE

    def peer(slot):
        px = (ix // 2 + slot // 4) % 2
        pc = (ix % 2 + slot % 2) % 2
        py = (iy + (slot // 2) % 2) % 2
        return px * 2 + pc, py

    def block_of(slot):
        return (slot + group - 1) % (2 * group - 1) + (group - slot) // group * (me - group + 1)

    def fetch(kind, head, slot, span=slice(None)):
        cx, cy = peer(slot)
        return pltpu.make_async_remote_copy(
            src_ref=pool.at[kind, cx * 2 + cy, head, span],
            dst_ref=pool.at[kind, group - 1 + slot, head, span],
            send_sem=send_sem.at[kind, head, slot],
            recv_sem=recv_sem.at[kind, head, slot],
            device_id=(batch, cy, cx),
            device_id_type=MESH,
        )

    def fetch_all(kind, head):
        for slot in SEND_ORDER:
            fetch(kind, head, slot).start()

    def give(head, slot):
        cx, cy = peer(slot)
        return pltpu.make_async_remote_copy(
            src_ref=pool.at[Q_IDX, block_of(slot), head],
            dst_ref=o_home.at[me, head],
            send_sem=send_sem.at[3, head, slot],
            recv_sem=recv_sem.at[3, head, slot],
            device_id=(batch, cy, cx),
            device_id_type=MESH,
        )

    def give_own(head):
        return pltpu.make_async_copy(pool.at[Q_IDX, me, head], o_home.at[me, head], recv_sem.at[3, head, 0])

    def token_span(tile):
        return pl.ds(pl.multiple_of(tile * LOAD_TILE, LOAD_TILE), LOAD_TILE)

    def load(kind, tile):
        return pltpu.make_async_copy(
            sources[kind].at[token_span(tile)], landing.at[tile % 2], load_sem.at[tile % 2]
        )

    load(K_IDX, 0).start()
    barrier = pltpu.get_barrier_semaphore()
    for slot in range(1, 8):
        cx, cy = peer(slot)
        pl.semaphore_signal(barrier, inc=1, device_id=(batch, cy, cx), device_id_type=MESH)

    def send_first(tile, count):
        for slot in SEND_ORDER:
            fetch(K_IDX, 0, slot, pl.ds(tile * LOAD_TILE, count * LOAD_TILE)).start()

    first_spans = [(0, 1)] + [(1 << n, 1 << n) for n in range(num_loads.bit_length() - 1)]

    for kind in (K_IDX, V_IDX, Q_IDX):

        def relayout(tile, carry):
            @pl.when(tile + 1 < num_loads)
            def _():
                load(kind, tile + 1).start()

            if kind != Q_IDX:

                @pl.when(tile + 1 == num_loads)
                def _():
                    load(kind + 1, 0).start()

            load(kind, tile).wait()

            def some_tokens(part, carry):
                rows = pl.ds(pl.multiple_of(part * TOKEN_GROUP, TOKEN_GROUP), TOKEN_GROUP)
                first = pl.multiple_of(tile * LOAD_TILE + part * TOKEN_GROUP, TOKEN_GROUP)
                by_head = jnp.swapaxes(landing[tile % 2, rows], 0, 1)
                pool[kind, :group, :, pl.ds(first, TOKEN_GROUP), :] = by_head.reshape(
                    group, heads, TOKEN_GROUP, head_dim
                )
                return carry

            lax.fori_loop(0, LOAD_TILE // TOKEN_GROUP, some_tokens, 0, unroll=LOAD_TILE // TOKEN_GROUP)

            if kind == K_IDX:

                @pl.when(tile == 1)
                def _():
                    pl.semaphore_wait(barrier, 7)

                for begin, count in first_spans[:-1]:

                    @pl.when(tile == begin + count)
                    def _():
                        send_first(begin, count)

            if kind == V_IDX:

                @pl.when(tile == 0)
                def _():
                    send_first(*first_spans[-1])

            return carry

        lax.fori_loop(0, num_loads, relayout, 0)

    for kind, head in ((V_IDX, 0), (Q_IDX, 0), (K_IDX, 1), (V_IDX, 1), (Q_IDX, 1)):
        fetch_all(kind, head)

    scale = math.log2(math.e) / math.sqrt(head_dim)
    per_slot = tokens // KV_TILE

    def rows(tile):
        return pl.ds(pl.multiple_of((tile % per_slot) * KV_TILE, KV_TILE), KV_TILE)

    def one_head(head, carry):
        for kind in (K_IDX, V_IDX):
            for slot in range(1, 8):
                fetch(kind, head, slot).wait_recv()

        @pl.when(head > 0)
        def _():
            give_own(head - 1).start()
            for slot in SEND_ORDER:
                give(head - 1, slot).start()

        def one_slot(turn, carry):
            slot = turn + head * (7 - 2 * turn)
            block = block_of(slot)

            @pl.when(slot != 0)
            def _():
                fetch(Q_IDX, head, slot).wait_recv()

            pool[Q_IDX, block, head] = attend(
                scale,
                lambda: pool[Q_IDX, block, head],
                lambda tile: pool[K_IDX, block_of(tile // per_slot), head, rows(tile), :],
                lambda tile: pool[V_IDX, block_of(tile // per_slot), head, rows(tile), :],
                group * per_slot,
                row_max,
                row_sum,
                out_acc,
                scores_buf,
            )

            @pl.when((head == heads - 1) & (slot == 0))
            def _():
                give_own(head).start()

            @pl.when((head == heads - 1) & (turn > 0))
            def _():
                give(head, slot + 1).start()

            return carry

        return lax.fori_loop(0, 8, one_slot, carry)

    lax.fori_loop(0, heads, one_head, 0)

    for head in range(heads):
        give_own(head).wait()
        for slot in range(1, 8):
            for kind in (K_IDX, V_IDX, Q_IDX):
                fetch(kind, head, slot).wait_send()
            give(head, slot).wait_send()
            give(head, slot).wait_recv()


def by_token(o_buf, out_hbm, out_buf, out_sem):
    num_tiles = o_buf.shape[1] // TOKEN_TILE

    def put(tile):
        span = pl.ds(pl.multiple_of(tile * TOKEN_TILE, TOKEN_TILE), TOKEN_TILE)
        return pltpu.make_async_copy(out_buf.at[span], out_hbm.at[span], out_sem.at[tile])

    def one_tile(tile, carry):
        def some_tokens(part, carry):
            rows = pl.ds(pl.multiple_of(tile * TOKEN_TILE + part * TOKEN_GROUP, TOKEN_GROUP), TOKEN_GROUP)
            out_buf[rows] = jnp.swapaxes(o_buf[:, rows], 0, 1)
            return carry

        lax.fori_loop(0, TOKEN_TILE // TOKEN_GROUP, some_tokens, 0, unroll=TOKEN_TILE // TOKEN_GROUP)
        put(tile).start()
        return carry

    lax.fori_loop(0, num_tiles, one_tile, 0)
    for tile in range(num_tiles):
        put(tile).wait()


def solution(mesh):
    group = mesh.shape["cx"] * mesh.shape["cy"]
    seq_spec = P(("batch", "cx", "cy"), None, None)

    def local_attention(q_local, k_local, v_local):
        tokens, num_heads, head_dim = q_local.shape
        heads = num_heads // group
        blocks = (group, heads, tokens, head_dim)
        anywhere = pl.BlockSpec(memory_space=pl.ANY)

        out = pl.pallas_call(
            kernel,
            out_shape=pltpu.VMEM(blocks, jnp.bfloat16),
            in_specs=[anywhere] * 3,
            out_specs=anywhere,
            scratch_shapes=[
                pltpu.VMEM((3, 2 * group - 1, heads, tokens, head_dim), jnp.bfloat16),
                pltpu.VMEM((2, LOAD_TILE, num_heads, head_dim), jnp.bfloat16),
                pltpu.VMEM((tokens, 128), jnp.float32),
                pltpu.VMEM((tokens, 128), jnp.float32),
                pltpu.VMEM((tokens, head_dim), jnp.float32),
                pltpu.VMEM((2, tokens, KV_TILE), jnp.float32),
                pltpu.SemaphoreType.DMA((4, heads, group)),
                pltpu.SemaphoreType.DMA((4, heads, group)),
                pltpu.SemaphoreType.DMA((2,)),
            ],
            compiler_params=pltpu.CompilerParams(
                collective_id=0, has_side_effects=True, vmem_limit_bytes=58600000
            ),
        )(k_local, v_local, q_local)
        return pl.pallas_call(
            by_token,
            out_shape=jax.ShapeDtypeStruct(q_local.shape, jnp.bfloat16),
            in_specs=[pl.BlockSpec(memory_space=pltpu.VMEM)],
            out_specs=anywhere,
            scratch_shapes=[
                pltpu.VMEM((tokens, num_heads, head_dim), jnp.bfloat16),
                pltpu.SemaphoreType.DMA((tokens // TOKEN_TILE,)),
            ],
            compiler_params=pltpu.CompilerParams(vmem_limit_bytes=24 * 2**20),
        )(out.reshape(num_heads, tokens, head_dim))

    return jax.shard_map(
        local_attention, mesh=mesh, in_specs=(seq_spec, seq_spec, seq_spec), out_specs=seq_spec, check_vma=False
    )
```
